32 devices in a mesh: facet: 4 (over z), chan: 8 (over y, x, core).
Axes of the slice: x: 2, y: 2, z: 4, core: 2. Of those that a mesh axis runs over, the one named last changes fastest.
Arguments:
- visibilities: bfloat16 [2, 8, 256, 32, 128], P(None, None, None, ('facet', 'chan')), may hold values from -12 to 12
- kernels: bfloat16 [32, 256, 512], replicated, may hold values from -0.25 to 0.25
- delays: float32 [8, 256, 128], P('facet'), may hold values from -4 to 4
- tile_of: int32 [8, 256], P('facet'), may hold values from 0 to 127
- plane_of: int32 [8, 256], P('facet'), may hold values from 0 to 31
- counts: int32 [8], P('facet'), may hold values from 64 to 256
- neighbours: int32 [8, 4], replicated, may hold values from 0 to 7, as said below
Outputs:
- joined_grids: float32 [128, 8, 4, 512], P('chan', 'facet')
The draws below stay inside these ranges and needn't reach their ends.
Inputs may be any that keep to these rules, and one draw needn't show every extreme that they name: `neighbours`: each row names 4 different facets, none of them its own.
All inputs are finite; a program needn't handle non-finite values.
Results may differ from the reference program's by a relative error of at most 0.0043.
Values may be sent and summed in bfloat16 or wider, within the bound.
A program may use at most 128 MiB of HBM per device.

```python
import math
import jax
import jax.numpy as jnp
from jax import lax

FACETS = 8
BLOCKS = 256
CHANNELS = 32
AVG = 8
OUTCH = 4
BV = 128
TS = 16
TILE = 256
NTILES = 128
WPLANES = 32
EDGE = 4
NNB = 4


def draw_neighbours(key, part):
    facet_keys = jax.random.split(jax.random.fold_in(key, 7), FACETS)

    def draw_row(row_key, facet_id):
        shuffled = jax.random.permutation(row_key, FACETS - 1)[:NNB].astype(jnp.int32)
        return jnp.where(shuffled >= facet_id, shuffled + 1, shuffled).astype(jnp.int32)
    return jax.vmap(draw_row)(facet_keys, jnp.arange(FACETS, dtype=jnp.int32))


def plant(result, stream_key, smallest, largest):
    place = [jax.random.randint(jax.random.fold_in(stream_key, axis), (), 0, length) for axis, length in enumerate(result.shape)]
    widest = result.shape.index(max(result.shape))
    beside = place[:widest] + [(place[widest] + 1) % result.shape[widest]] + place[widest + 1:]
    return result.at[tuple(place)].set(smallest).at[tuple(beside)].set(largest)


def levels(key, dims, pieces, least, top_value):
    gain = 1.0
    for dim, blocks in pieces:
        heights = jax.random.uniform(jax.random.fold_in(jax.random.fold_in(key, 6), dim), (blocks,), jnp.float32, least / len(pieces), top_value / len(pieces))
        gain = gain * jnp.repeat(jnp.exp(heights), dims[dim] // blocks).reshape((-1,) + (1,) * (len(dims) - 1 - dim))
    return gain


def bell_draw(own_key, extent, spread, reach, pieces=(), kind=jnp.bfloat16):
    array = spread * jax.random.normal(own_key, extent, jnp.float32)
    if pieces:
        array = array * levels(own_key, extent, pieces, -0.22, 0.18)
    return jnp.clip(array, -reach, reach).astype(kind)


def setup_inputs(seed: int = 0) -> dict:
    arg_keys = jax.random.split(jax.random.key(seed), 8)
    return {
        "visibilities": bell_draw(arg_keys[0], (2, FACETS, BLOCKS, CHANNELS, BV), 2.0, 12.0, ((3, 32),)),
        "kernels": bell_draw(arg_keys[1], (WPLANES, 2 * BV, 2 * TILE), (2 * BV * BLOCKS // NTILES) ** -0.5, 0.25),
        "delays": jnp.clip(jax.random.uniform(arg_keys[2], (FACETS, BLOCKS, BV), jnp.float32, -4.0, 4.0) * levels(arg_keys[2], (FACETS, BLOCKS, BV), ((0, 4),), -0.4, 0.0), -4.0, 4.0),
        "tile_of": plant(jax.random.randint(arg_keys[3], (FACETS, BLOCKS), 0, NTILES), jax.random.fold_in(arg_keys[3], 1), 0, NTILES - 1).astype(jnp.int32),
        "plane_of": plant(jax.random.randint(arg_keys[4], (FACETS, BLOCKS), 0, WPLANES), jax.random.fold_in(arg_keys[4], 1), 0, WPLANES - 1).astype(jnp.int32),
        "counts": plant(jax.random.randint(arg_keys[5], (FACETS,), BLOCKS // 4, BLOCKS + 1), jax.random.fold_in(arg_keys[5], 1), BLOCKS // 4, BLOCKS).astype(jnp.int32),
        "neighbours": draw_neighbours(jax.random.fold_in(arg_keys[7], 71), 0),
    }


def reference(visibilities, kernels, delays, tile_of, plane_of, counts, neighbours):
    highest = lax.Precision.HIGHEST
    channel = jnp.arange(CHANNELS, dtype=jnp.float32)
    freq_turn = (2.0 * math.pi) * (1.0 + 0.5 * channel / CHANNELS)
    group_rows = math.gcd(BLOCKS, 64)

    def grid_facet(facet_id):
        vis_facet = lax.dynamic_index_in_dim(visibilities, facet_id, 1, keepdims=False)
        delay_facet = lax.dynamic_index_in_dim(delays, facet_id, 0, keepdims=False)
        tiles_facet = lax.dynamic_index_in_dim(tile_of, facet_id, 0, keepdims=False)
        planes_facet = lax.dynamic_index_in_dim(plane_of, facet_id, 0, keepdims=False)
        live_count = lax.dynamic_index_in_dim(counts, facet_id, 0, keepdims=False)

        def one_group(grid_acc, group_index):
            begin_row = (group_index * group_rows).astype(jnp.int32)
            vis_piece = lax.dynamic_slice_in_dim(vis_facet, begin_row, group_rows, 1).astype(jnp.float32)
            delay_piece = lax.dynamic_slice_in_dim(delay_facet, begin_row, group_rows, 0)
            phase_angle = delay_piece[:, None, :] * freq_turn[None, :, None]
            cosine = jnp.cos(phase_angle)
            sine_part = jnp.sin(phase_angle)
            rot_real = vis_piece[0] * cosine - vis_piece[1] * sine_part
            rot_imag = vis_piece[0] * sine_part + vis_piece[1] * cosine
            avg_real = jnp.mean(rot_real.reshape(group_rows, OUTCH, AVG, BV), axis=2)
            avg_imag = jnp.mean(rot_imag.reshape(group_rows, OUTCH, AVG, BV), axis=2)
            avg_rows = jnp.concatenate([avg_real, avg_imag], axis=-1).astype(jnp.bfloat16)
            plane_piece = lax.dynamic_slice_in_dim(planes_facet, begin_row, group_rows, 0).astype(jnp.int32)
            chosen = jnp.take(kernels, plane_piece, axis=0)
            contrib = jnp.einsum("gcv,gvx->gcx", avg_rows.astype(jnp.float32), chosen.astype(jnp.float32), precision=highest)
            block_ids = begin_row + jnp.arange(group_rows, dtype=jnp.int32)
            live_mask = (block_ids < live_count).astype(jnp.float32)
            tile_piece = lax.dynamic_slice_in_dim(tiles_facet, begin_row, group_rows, 0).astype(jnp.int32)
            grid_acc = grid_acc.at[tile_piece].add(contrib * live_mask[:, None, None])
            return grid_acc, None

        start_grid = jnp.zeros((NTILES, OUTCH, 2 * TILE), jnp.float32)
        grid_acc, unused = lax.scan(one_group, start_grid, jnp.arange(BLOCKS // group_rows, dtype=jnp.int32))
        return grid_acc

    facet_grids = lax.map(grid_facet, jnp.arange(FACETS, dtype=jnp.int32))
    facet_grids = jnp.transpose(facet_grids, (1, 0, 2, 3))
    edge_cells = EDGE * TS
    strips = jnp.concatenate([facet_grids[..., :edge_cells], facet_grids[..., TILE:TILE + edge_cells]], axis=-1)
    neighbour_strips = jnp.take(strips, neighbours.astype(jnp.int32), axis=1)
    blended = 0.25 * jnp.sum(neighbour_strips, axis=2)
    joined = facet_grids.at[..., TILE - edge_cells:TILE].add(blended[..., :edge_cells])
    joined = joined.at[..., 2 * TILE - edge_cells:].add(blended[..., edge_cells:])
    return joined
```

```python
import functools
import math

import jax
import jax.numpy as jnp
from jax import lax
from jax.experimental import pallas as pl
from jax.experimental.pallas import tpu as pltpu
from jax.sharding import PartitionSpec as P

AVG = 8
TS = 16
NT_DEV = 16
EDGE = 4
LANES = 128
MESH = pl.DeviceIdType.MESH


def series(first, count, scale):
    return [
        (-1.0) ** i * scale ** (2 * i + first) / math.factorial(2 * i + first)
        for i in range(count)
    ]


SIN_HALF = series(1, 7, math.pi)
COS_HALF = series(0, 7, math.pi)


def turn_parts(turns):
    frac = turns - jnp.round(turns)
    square = frac * frac
    sine = jnp.full_like(frac, SIN_HALF[-1])
    cosine = jnp.full_like(frac, COS_HALF[-1])
    for a, b in zip(SIN_HALF[-2::-1], COS_HALF[-2::-1]):
        sine = sine * square + a
        cosine = cosine * square + b
    sine = sine * frac
    return 1.0 - 2.0 * sine * sine, 2.0 * sine * cosine


def kernel(
    cfg,
    neigh_ref,
    vis_ref,
    delay_ref,
    code_ref,
    kern_ref,
    out_ref,
    got,
    turns,
    codes,
    rows,
    kern,
    lhs,
    grid,
    final,
    vis_send,
    vis_recv,
    turn_send,
    turn_recv,
    code_send,
    code_recv,
    row_send,
    row_recv,
    relay_send,
    relay_recv,
    fin_send,
    fin_recv,
    own_sem,
    kern_sem,
):
    n, nz, facets, fac, blk, groups, planes, tiles, chunks = cfg
    me = lax.axis_index("chan")
    zme = lax.axis_index("facet")
    channels = groups * AVG * nz
    cells = kern_ref.shape[1]
    tile = cells // 2
    edge = EDGE * TS
    per = facets // chunks
    pairs = n // 2
    mate = me + 1 - 2 * lax.rem(me, 2)
    parity = lax.rem(me, 2)
    my_pair = me // 2

    load_kern = pltpu.make_async_copy(kern_ref, kern, kern_sem)
    load_kern.start()

    barrier = pltpu.get_barrier_semaphore()
    for d in range(1, n):
        pl.semaphore_signal(
            barrier, inc=1, device_id={"chan": lax.rem(me + d, n)}, device_id_type=MESH
        )
    for d in range(1, nz):
        pl.semaphore_signal(
            barrier, inc=1, device_id={"facet": lax.rem(zme + d, nz)}, device_id_type=MESH
        )

    my_blocks = pl.ds(pl.multiple_of(me * blk, blk), blk)
    my_facets = pl.ds(zme * fac, fac)

    def own_copy(c):
        return pltpu.make_async_copy(
            vis_ref.at[:, pl.ds(c * per, per), my_blocks],
            got.at[me, :, pl.ds(c * per, per)],
            own_sem.at[c],
        )

    own_turns = pltpu.make_async_copy(
        delay_ref.at[:, my_blocks], turns.at[my_facets], own_sem.at[chunks]
    )
    own_codes = pltpu.make_async_copy(code_ref, codes.at[my_facets], own_sem.at[chunks + 1])
    for c in range(chunks):
        own_copy(c).start()
    own_turns.start()
    own_codes.start()
    pl.semaphore_wait(barrier, n + nz - 2)

    def vis_copy(peer, slot, c, d):
        return pltpu.make_async_remote_copy(
            src_ref=vis_ref.at[:, pl.ds(c * per, per), pl.ds(pl.multiple_of(peer * blk, blk), blk)],
            dst_ref=got.at[slot, :, pl.ds(c * per, per)],
            send_sem=vis_send.at[d, c],
            recv_sem=vis_recv.at[d, c],
            device_id={"chan": peer},
            device_id_type=MESH,
        )

    def turn_copy(peer, slot, d):
        return pltpu.make_async_remote_copy(
            src_ref=delay_ref.at[:, my_blocks],
            dst_ref=turns.at[pl.ds(slot * fac, fac)],
            send_sem=turn_send.at[d],
            recv_sem=turn_recv.at[d],
            device_id={"facet": peer},
            device_id_type=MESH,
        )

    def code_copy(peer, slot, d):
        return pltpu.make_async_remote_copy(
            src_ref=code_ref,
            dst_ref=codes.at[pl.ds(slot * fac, fac)],
            send_sem=code_send.at[d],
            recv_sem=code_recv.at[d],
            device_id={"facet": peer},
            device_id_type=MESH,
        )

    for d in range(1, nz):
        turn_copy(lax.rem(zme + d, nz), zme, d).start()
    for c in range(chunks):
        for d in range(1, n):
            vis_copy(lax.rem(me + d, n), me, c, d).start()
    for d in range(1, nz):
        code_copy(lax.rem(zme + d, nz), zme, d).start()

    def row_copy(owner, peer, c, send, recv):
        part = rows.at[
            pl.ds(c * per, per), pl.ds(pl.multiple_of(owner * blk, blk), blk)
        ]
        return pltpu.make_async_remote_copy(
            src_ref=part,
            dst_ref=part,
            send_sem=send,
            recv_sem=recv,
            device_id={"chan": peer},
            device_id_type=MESH,
        )

    own_turns.wait()
    for d in range(1, nz):
        turn_copy(lax.rem(zme + d, nz), lax.rem(zme + nz - d, nz), d).wait_recv()

    for c in range(chunks):
        own_copy(c).wait()
        for d in range(1, n):
            vis_copy(lax.rem(me + d, n), lax.rem(me + n - d, n), c, d).wait_recv()

        def rotate(i, carry):
            f = c * per + i
            delay = turns[f]
            step_cos, step_sin = turn_parts(delay * (0.5 / channels))
            for g in range(groups):
                first = (zme * groups + g) * AVG
                start_cos, start_sin = turn_parts(
                    delay * (1.0 + (0.5 / channels) * first.astype(jnp.float32))
                )
                real = got[g * AVG + AVG - 1, 0, f].astype(jnp.float32)
                imag = got[g * AVG + AVG - 1, 1, f].astype(jnp.float32)
                for k in range(AVG - 2, -1, -1):
                    next_real = got[g * AVG + k, 0, f].astype(jnp.float32) + (
                        real * step_cos - imag * step_sin
                    )
                    imag = got[g * AVG + k, 1, f].astype(jnp.float32) + (
                        real * step_sin + imag * step_cos
                    )
                    real = next_real
                rows[f, my_blocks, 2 * LANES * g : 2 * LANES * g + LANES] = (
                    (real * start_cos - imag * start_sin) * (1.0 / AVG)
                ).astype(jnp.bfloat16)
                rows[f, my_blocks, 2 * LANES * g + LANES : 2 * LANES * (g + 1)] = (
                    (real * start_sin + imag * start_cos) * (1.0 / AVG)
                ).astype(jnp.bfloat16)
            return carry

        lax.fori_loop(0, per, rotate, 0)
        for q in range(1, pairs):
            peer = 2 * lax.rem(my_pair + q, pairs) + parity
            row_copy(me, peer, c, row_send.at[q, c], row_recv.at[q, c]).start()
        row_copy(me, mate, c, row_send.at[0, c], row_recv.at[0, c]).start()

    own_codes.wait()
    for d in range(1, nz):
        code_copy(lax.rem(zme + d, nz), lax.rem(zme + nz - d, nz), d).wait_recv()

    for c in range(chunks):
        for q in range(1, pairs):
            owner = 2 * lax.rem(my_pair + pairs - q, pairs) + parity
            row_copy(owner, mate, c, row_send.at[q, c], row_recv.at[q, c]).wait_recv()
            row_copy(owner, mate, c, relay_send.at[q, c], relay_recv.at[q, c]).start()

    entry = lax.broadcasted_iota(jnp.int32, (planes * NT_DEV, blk * n), 0)
    wanted = (entry // NT_DEV) * tiles + me * NT_DEV + lax.rem(entry, NT_DEV)
    for c in range(chunks):
        row_copy(mate, mate, c, row_send.at[0, c], row_recv.at[0, c]).wait_recv()
        for q in range(1, pairs):
            owner = 2 * lax.rem(my_pair + pairs - q, pairs) + 1 - parity
            row_copy(owner, mate, c, relay_send.at[q, c], relay_recv.at[q, c]).wait_recv()

        for i in range(per):
            f = c * per + i
            table = (codes[f] == wanted).astype(jnp.float32).astype(jnp.bfloat16)
            summed = jnp.dot(table, rows[f], preferred_element_type=jnp.float32).astype(
                jnp.bfloat16
            )
            for g in range(groups):
                at = (g * facets + f) * NT_DEV
                for p in range(planes):
                    lhs[at : at + NT_DEV, 2 * LANES * p : 2 * LANES * (p + 1)] = summed[
                        p * NT_DEV : (p + 1) * NT_DEV, 2 * LANES * g : 2 * LANES * (g + 1)
                    ]

    load_kern.wait()
    grid[...] = jnp.dot(lhs[...], kern[...], preferred_element_type=jnp.float32)

    span = facets * NT_DEV
    row_id = lax.broadcasted_iota(jnp.int32, (NT_DEV, span), 0)
    col_id = lax.broadcasted_iota(jnp.int32, (NT_DEV, span), 1)
    same_tile = lax.rem(col_id, NT_DEV) == row_id
    col_facet = col_id // NT_DEV
    parts = []
    for f in range(facets):
        weight = jnp.zeros((NT_DEV, span), jnp.float32)
        for k in range(neigh_ref.shape[1]):
            weight += jnp.where(same_tile & (col_facet == neigh_ref[f, k]), 0.25, 0.0)
        parts.append(weight)
    mix = jnp.concatenate(parts, axis=0).astype(jnp.bfloat16)
    keep = lax.broadcasted_iota(jnp.int32, (span, LANES), 1) >= LANES - edge
    for g in range(groups):
        here = slice(g * span, (g + 1) * span)
        for half in range(2):
            base = half * tile
            strip = grid[here, base : base + LANES].astype(jnp.bfloat16)
            blended = jnp.dot(mix, strip, preferred_element_type=jnp.float32)
            moved = pltpu.roll(blended, LANES - edge, 1)
            last = slice(base + tile - LANES, base + tile)
            grid[here, last] += jnp.where(keep, moved, 0.0)
    for z in range(nz):
        for g in range(groups):
            at = (g * facets + z * fac) * NT_DEV
            final[z, g] = grid[at : at + fac * NT_DEV].astype(jnp.bfloat16)

    def fin_copy(peer, slot, d):
        return pltpu.make_async_remote_copy(
            src_ref=final.at[peer],
            dst_ref=out_ref.at[slot],
            send_sem=fin_send.at[d],
            recv_sem=fin_recv.at[d],
            device_id={"facet": peer},
            device_id_type=MESH,
        )

    for d in range(1, nz):
        fin_copy(lax.rem(zme + d, nz), zme, d).start()
    out_ref[zme] = final[zme]

    for d in range(1, nz):
        turn_copy(lax.rem(zme + d, nz), zme, d).wait_send()
        code_copy(lax.rem(zme + d, nz), zme, d).wait_send()
    for c in range(chunks):
        for d in range(1, n):
            vis_copy(lax.rem(me + d, n), me, c, d).wait_send()
        for q in range(pairs):
            row_copy(me, mate, c, row_send.at[q, c], row_recv.at[q, c]).wait_send()
        for q in range(1, pairs):
            row_copy(me, mate, c, relay_send.at[q, c], relay_recv.at[q, c]).wait_send()
    for d in range(1, nz):
        fin_copy(lax.rem(zme + d, nz), zme, d).wait_send()
        fin_copy(lax.rem(zme + d, nz), lax.rem(zme + nz - d, nz), d).wait_recv()


CHUNKS = 2


def local(visibilities, kernels, delays, tile_of, plane_of, counts, neighbours):
    n = lax.axis_size("chan")
    nz = lax.axis_size("facet")
    halves, facets, blocks, ch_dev, lanes = visibilities.shape
    planes, depth, cells = kernels.shape
    fac = facets // nz
    blk = blocks // n
    groups = n * ch_dev // AVG
    tiles = NT_DEV * n
    chunks = CHUNKS
    vis = visibilities.reshape(halves, facets, blocks, lanes)
    block_id = jnp.arange(blocks, dtype=jnp.int32)[None, :]
    code = jnp.where(block_id < counts[:, None], plane_of * tiles + tile_of, -1)
    code = code.reshape(fac, 1, blocks)
    cfg = (n, nz, facets, fac, blk, groups, planes, tiles, chunks)
    dma = pltpu.SemaphoreType.DMA
    span = facets * NT_DEV
    out = pl.pallas_call(
        functools.partial(kernel, cfg),
        out_shape=jax.ShapeDtypeStruct((nz, groups, fac * NT_DEV, cells), jnp.bfloat16),
        in_specs=[
            pl.BlockSpec(memory_space=pltpu.SMEM),
            pl.BlockSpec(memory_space=pl.ANY),
            pl.BlockSpec(memory_space=pl.ANY),
            pl.BlockSpec(memory_space=pltpu.VMEM),
            pl.BlockSpec(memory_space=pl.ANY),
        ],
        out_specs=pl.BlockSpec(memory_space=pltpu.VMEM),
        scratch_shapes=[
            pltpu.VMEM((n, halves, facets, blk, lanes), jnp.bfloat16),
            pltpu.VMEM((facets, blk, lanes), jnp.float32),
            pltpu.VMEM((facets, 1, blocks), jnp.int32),
            pltpu.VMEM((facets, blocks, groups * depth), jnp.bfloat16),
            pltpu.VMEM((planes * depth, cells), jnp.bfloat16),
            pltpu.VMEM((groups * span, planes * depth), jnp.bfloat16),
            pltpu.VMEM((groups * span, cells), jnp.float32),
            pltpu.VMEM((nz, groups, fac * NT_DEV, cells), jnp.bfloat16),
            dma((n, chunks)),
            dma((n, chunks)),
            dma((nz,)),
            dma((nz,)),
            dma((nz,)),
            dma((nz,)),
            dma((n // 2, chunks)),
            dma((n // 2, chunks)),
            dma((n // 2, chunks)),
            dma((n // 2, chunks)),
            dma((nz,)),
            dma((nz,)),
            dma((chunks + 2,)),
            dma,
        ],
        compiler_params=pltpu.CompilerParams(
            collective_id=0, has_side_effects=True, vmem_limit_bytes=60 * 1024 * 1024
        ),
    )(neighbours, vis, delays, code, kernels.reshape(planes * depth, cells))
    spread = out.reshape(nz * groups, fac, NT_DEV, cells).astype(jnp.float32)
    return jnp.transpose(spread, (2, 1, 0, 3))


def solution(mesh):
    return jax.shard_map(
        local,
        mesh=mesh,
        in_specs=(
            P(None, None, None, ("facet", "chan"), None),
            P(),
            P("facet", None, None),
            P("facet", None),
            P("facet", None),
            P("facet"),
            P(),
        ),
        out_specs=P("chan", "facet", None, None),
        check_vma=False,
    )
```

```python
import functools
import math

import jax
import jax.numpy as jnp
from jax import lax
from jax.experimental import pallas as pl
from jax.experimental.pallas import tpu as pltpu
from jax.sharding import PartitionSpec as P

AVG = 8
TS = 16
NT_DEV = 16
EDGE = 4
LANES = 128
MESH = pl.DeviceIdType.MESH


def series(first, count, scale):
    return [
        (-1.0) ** i * scale ** (2 * i + first) / math.factorial(2 * i + first)
        for i in range(count)
    ]


SIN_HALF = series(1, 7, math.pi)
COS_HALF = series(0, 7, math.pi)


def turn_parts(turns):
    frac = turns - jnp.round(turns)
    square = frac * frac
    sine = jnp.full_like(frac, SIN_HALF[-1])
    cosine = jnp.full_like(frac, COS_HALF[-1])
    for a, b in zip(SIN_HALF[-2::-1], COS_HALF[-2::-1]):
        sine = sine * square + a
        cosine = cosine * square + b
    sine = sine * frac
    return 1.0 - 2.0 * sine * sine, 2.0 * sine * cosine


def flip(index, mask):
    bit = 1
    while bit <= mask:
        if mask & bit:
            index = index + bit - 2 * bit * lax.rem(index // bit, 2)
        bit *= 2
    return index


def kernel(
    cfg,
    neigh_ref,
    count_ref,
    vis_ref,
    delay_ref,
    tile_ref,
    plane_ref,
    kern_ref,
    out_ref,
    pair,
    part,
    got,
    wide,
    rough,
    turns,
    codes,
    rows,
    kern,
    lhs,
    grid,
    final,
    mate_send,
    mate_recv,
    rough_send,
    rough_recv,
    turn_send,
    turn_recv,
    code_send,
    code_recv,
    part_send,
    part_recv,
    row_send,
    row_recv,
    relay_send,
    relay_recv,
    fin_send,
    fin_recv,
    own_sem,
    kern_sem,
):
    n, nz, facets, fac, blk, groups, planes, tiles = cfg
    me = lax.axis_index("chan")
    zme = lax.axis_index("facet")
    channels = groups * AVG * nz
    tile = kern_ref.shape[1] // 2
    edge = EDGE * TS
    pairs = n // 2
    parity = lax.rem(me, 2)
    mate = me + 1 - 2 * parity
    my_pair = me // 2
    half_avg = AVG // 2
    chunk_z = [flip(zme, c) for c in range(nz)]

    def group_of(c):
        return pl.ds(chunk_z[c] * fac, fac)

    load_kern = pltpu.make_async_copy(kern_ref, kern, kern_sem)
    own_wide = pltpu.make_async_copy(delay_ref.at[:, :, parity], wide, own_sem.at[nz])
    own_turns = pltpu.make_async_copy(
        delay_ref.at[:, my_pair, parity], turns.at[zme], own_sem.at[nz + 1]
    )

    def own_copy(c):
        return pltpu.make_async_copy(
            vis_ref.at[:, group_of(c), :, parity],
            pair.at[parity, :, group_of(c)],
            own_sem.at[c],
        )

    barrier = pltpu.get_barrier_semaphore()
    for d in range(1, n):
        pl.semaphore_signal(
            barrier, inc=1, device_id={"chan": lax.rem(me + d, n)}, device_id_type=MESH
        )
    for d in range(1, nz):
        pl.semaphore_signal(
            barrier, inc=1, device_id={"facet": chunk_z[d]}, device_id_type=MESH
        )
    own_wide.start()
    for c in range(nz):
        own_copy(c).start()
    own_turns.start()
    load_kern.start()

    blocks = blk * n
    block_id = lax.broadcasted_iota(jnp.int32, (1, blocks), 1)
    for i in range(fac):
        codes[zme, i : i + 1] = jnp.where(
            block_id < count_ref[i],
            plane_ref[i : i + 1] * tiles + tile_ref[i : i + 1],
            -1,
        )
    own_wide.wait()
    rough[zme] = wide[...].astype(jnp.bfloat16)
    pl.semaphore_wait(barrier, n + nz - 2)

    def mate_copy(c, slot):
        return pltpu.make_async_remote_copy(
            src_ref=vis_ref.at[:, group_of(c), :, 1 - parity],
            dst_ref=pair.at[slot, :, group_of(c)],
            send_sem=mate_send.at[c],
            recv_sem=mate_recv.at[c],
            device_id={"chan": mate},
            device_id_type=MESH,
        )

    def facet_copy(src, buffer, slot, d, send, recv):
        return pltpu.make_async_remote_copy(
            src_ref=src,
            dst_ref=buffer.at[slot],
            send_sem=send.at[d],
            recv_sem=recv.at[d],
            device_id={"facet": chunk_z[d]},
            device_id_type=MESH,
        )

    def rough_copy(d, slot):
        return facet_copy(rough.at[zme], rough, slot, d, rough_send, rough_recv)

    def turn_copy(d, slot):
        return facet_copy(
            delay_ref.at[:, my_pair, parity], turns, slot, d, turn_send, turn_recv
        )

    def code_copy(d, slot):
        return facet_copy(codes.at[zme], codes, slot, d, code_send, code_recv)

    for c in range(nz):
        mate_copy(c, parity).start()
    for d in range(1, nz):
        turn_copy(d, zme).start()
    for d in range(1, nz):
        rough_copy(d, zme).start()
    for d in range(1, nz):
        code_copy(d, zme).start()

    my_blocks = pl.ds(pl.multiple_of(me * blk, blk), blk)

    def part_copy(c, d, owner, slot):
        return pltpu.make_async_remote_copy(
            src_ref=part.at[owner, :, group_of(c)],
            dst_ref=got.at[slot, :, group_of(c)],
            send_sem=part_send.at[d, c],
            recv_sem=part_recv.at[d, c],
            device_id={"chan": 2 * owner + parity},
            device_id_type=MESH,
        )

    def row_copy(owner, peer, c, send, recv):
        piece = rows.at[group_of(c), pl.ds(pl.multiple_of(owner * blk, blk), blk)]
        return pltpu.make_async_remote_copy(
            src_ref=piece,
            dst_ref=piece,
            send_sem=send,
            recv_sem=recv,
            device_id={"chan": peer},
            device_id_type=MESH,
        )

    def after(d):
        return lax.rem(my_pair + d, pairs)

    def before(d):
        return lax.rem(my_pair + pairs - d, pairs)

    def join_pair(c):
        own_copy(c).wait()
        mate_copy(c, 1 - parity).wait_recv()
        if c:
            rough_copy(c, chunk_z[c]).wait_recv()

        def one(i, carry):
            slot = i // pairs
            q = lax.rem(i, pairs)
            f = chunk_z[c] * fac + slot
            cosine, sine = turn_parts(
                rough[chunk_z[c], slot, q].astype(jnp.float32) * (0.5 / channels)
            )
            real = pair[1, 0, f, q].astype(jnp.float32)
            imag = pair[1, 1, f, q].astype(jnp.float32)
            part[q, 0, f] = (
                pair[0, 0, f, q].astype(jnp.float32) + (real * cosine - imag * sine)
            ).astype(jnp.bfloat16)
            part[q, 1, f] = (
                pair[0, 1, f, q].astype(jnp.float32) + (real * sine + imag * cosine)
            ).astype(jnp.bfloat16)
            return carry

        lax.fori_loop(0, fac * pairs, one, 0)
        for d in range(1, pairs):
            part_copy(c, d, after(d), my_pair).start()
        got[my_pair, :, group_of(c)] = part[my_pair, :, group_of(c)]

    def rotate(c):
        if c:
            turn_copy(c, chunk_z[c]).wait_recv()
        else:
            own_turns.wait()
        for d in range(1, pairs):
            part_copy(c, d, after(d), before(d)).wait_recv()

        def one(i, carry):
            f = chunk_z[c] * fac + i
            delay = turns[chunk_z[c], i]
            step_cos, step_sin = turn_parts(delay * (1.0 / channels))
            for g in range(groups):
                first = (zme * groups + g) * AVG
                start_cos, start_sin = turn_parts(
                    delay * (1.0 + (0.5 / channels) * first.astype(jnp.float32))
                )
                top = (g + 1) * half_avg - 1
                real = got[top, 0, f].astype(jnp.float32)
                imag = got[top, 1, f].astype(jnp.float32)
                for k in range(top - 1, g * half_avg - 1, -1):
                    next_real = got[k, 0, f].astype(jnp.float32) + (
                        real * step_cos - imag * step_sin
                    )
                    imag = got[k, 1, f].astype(jnp.float32) + (
                        real * step_sin + imag * step_cos
                    )
                    real = next_real
                rows[f, my_blocks, 2 * LANES * g : 2 * LANES * g + LANES] = (
                    (real * start_cos - imag * start_sin) * (1.0 / AVG)
                ).astype(jnp.bfloat16)
                rows[f, my_blocks, 2 * LANES * g + LANES : 2 * LANES * (g + 1)] = (
                    (real * start_sin + imag * start_cos) * (1.0 / AVG)
                ).astype(jnp.bfloat16)
            return carry

        lax.fori_loop(0, fac, one, 0)
        for q in range(1, pairs):
            row_copy(me, 2 * after(q) + parity, c, row_send.at[q, c], row_recv.at[q, c]).start()
        row_copy(me, mate, c, row_send.at[0, c], row_recv.at[0, c]).start()

    def relay(c):
        for q in range(1, pairs):
            owner = 2 * before(q) + parity
            row_copy(owner, mate, c, row_send.at[q, c], row_recv.at[q, c]).wait_recv()
            row_copy(owner, mate, c, relay_send.at[q, c], relay_recv.at[q, c]).start()

    entry = lax.broadcasted_iota(jnp.int32, (planes * NT_DEV, blocks), 0)
    wanted = (entry // NT_DEV) * tiles + me * NT_DEV + lax.rem(entry, NT_DEV)

    def gather_rows(c):
        if c:
            code_copy(c, chunk_z[c]).wait_recv()
        row_copy(mate, mate, c, row_send.at[0, c], row_recv.at[0, c]).wait_recv()
        for q in range(1, pairs):
            owner = 2 * before(q) + 1 - parity
            row_copy(owner, mate, c, relay_send.at[q, c], relay_recv.at[q, c]).wait_recv()
        for i in range(fac):
            f = chunk_z[c] * fac + i
            code = codes[chunk_z[c], i : i + 1]
            table = (code == wanted).astype(jnp.float32).astype(jnp.bfloat16)
            summed = jnp.dot(table, rows[f], preferred_element_type=jnp.float32).astype(
                jnp.bfloat16
            )
            for g in range(groups):
                at = pl.ds(pl.multiple_of((g * facets + f) * NT_DEV, NT_DEV), NT_DEV)
                for p in range(planes):
                    lhs[at, 2 * LANES * p : 2 * LANES * (p + 1)] = summed[
                        p * NT_DEV : (p + 1) * NT_DEV, 2 * LANES * g : 2 * LANES * (g + 1)
                    ]

    stages = (join_pair, rotate, relay, gather_rows)
    for step in range(nz + len(stages) - 1):
        for lag, stage in enumerate(stages):
            if 0 <= step - lag < nz:
                stage(step - lag)

    span = facets * NT_DEV
    row_id = lax.broadcasted_iota(jnp.int32, (NT_DEV, span), 0)
    col_id = lax.broadcasted_iota(jnp.int32, (NT_DEV, span), 1)
    same_tile = lax.rem(col_id, NT_DEV) == row_id
    col_facet = col_id // NT_DEV
    weights = []
    for f in range(facets):
        weight = jnp.zeros((NT_DEV, span), jnp.float32)
        for k in range(neigh_ref.shape[0]):
            weight += jnp.where(same_tile & (col_facet == neigh_ref[k, f]), 0.25, 0.0)
        weights.append(weight)
    mix = jnp.concatenate(weights, axis=0).astype(jnp.bfloat16)
    keep = lax.broadcasted_iota(jnp.int32, (span, LANES), 1) >= LANES - edge

    def fin_copy(half, d, slot):
        return pltpu.make_async_remote_copy(
            src_ref=final.at[half, chunk_z[d]],
            dst_ref=out_ref.at[slot, :, :, pl.ds(half * tile, tile)],
            send_sem=fin_send.at[d, half],
            recv_sem=fin_recv.at[d, half],
            device_id={"facet": chunk_z[d]},
            device_id_type=MESH,
        )

    load_kern.wait()
    for half in range(2):
        grid[...] = jnp.dot(
            lhs[...],
            kern[:, half * tile : (half + 1) * tile],
            preferred_element_type=jnp.float32,
        )
        for g in range(groups):
            here = slice(g * span, (g + 1) * span)
            blended = jnp.dot(
                mix, grid[here, :LANES].astype(jnp.bfloat16), preferred_element_type=jnp.float32
            )
            moved = pltpu.roll(blended, LANES - edge, 1)
            grid[here, tile - LANES :] += jnp.where(keep, moved, 0.0)
        for z in range(nz):
            for g in range(groups):
                at = (g * facets + z * fac) * NT_DEV
                final[half, z, g] = grid[at : at + fac * NT_DEV].astype(jnp.bfloat16)
        for d in range(1, nz):
            fin_copy(half, d, zme).start()
        out_ref[zme, :, :, half * tile : (half + 1) * tile] = final[half, zme]

    for c in range(nz):
        mate_copy(c, parity).wait_send()
        for q in range(pairs):
            row_copy(me, mate, c, row_send.at[q, c], row_recv.at[q, c]).wait_send()
        for q in range(1, pairs):
            part_copy(c, q, after(q), my_pair).wait_send()
            row_copy(me, mate, c, relay_send.at[q, c], relay_recv.at[q, c]).wait_send()
    for d in range(1, nz):
        turn_copy(d, zme).wait_send()
        rough_copy(d, zme).wait_send()
        code_copy(d, zme).wait_send()
    for half in range(2):
        for d in range(1, nz):
            fin_copy(half, d, zme).wait_send()
            fin_copy(half, d, chunk_z[d]).wait_recv()


def local(visibilities, kernels, delays, tile_of, plane_of, counts, neighbours):
    n = lax.axis_size("chan")
    nz = lax.axis_size("facet")
    halves, facets, blocks, ch_dev, lanes = visibilities.shape
    planes, depth, cells = kernels.shape
    fac = facets // nz
    blk = blocks // n
    pairs = n // 2
    groups = n * ch_dev // AVG
    tiles = NT_DEV * n
    vis = visibilities.reshape(halves, facets, pairs, 2, blk, lanes)
    cfg = (n, nz, facets, fac, blk, groups, planes, tiles)
    dma = pltpu.SemaphoreType.DMA
    span = facets * NT_DEV
    smem = pl.BlockSpec(memory_space=pltpu.SMEM)
    vmem = pl.BlockSpec(memory_space=pltpu.VMEM)
    anywhere = pl.BlockSpec(memory_space=pl.ANY)
    out = pl.pallas_call(
        functools.partial(kernel, cfg),
        out_shape=jax.ShapeDtypeStruct((nz, groups, fac * NT_DEV, cells), jnp.bfloat16),
        in_specs=[smem, smem, anywhere, anywhere, vmem, vmem, anywhere],
        out_specs=vmem,
        scratch_shapes=[
            pltpu.VMEM((2, halves, facets, pairs, blk, lanes), jnp.bfloat16),
            pltpu.VMEM((pairs, halves, facets, blk, lanes), jnp.bfloat16),
            pltpu.VMEM((pairs, halves, facets, blk, lanes), jnp.bfloat16),
            pltpu.VMEM((fac, pairs, blk, lanes), jnp.float32),
            pltpu.VMEM((nz, fac, pairs, blk, lanes), jnp.bfloat16),
            pltpu.VMEM((nz, fac, blk, lanes), jnp.float32),
            pltpu.VMEM((nz, fac, blocks), jnp.int32),
            pltpu.VMEM((facets, blocks, groups * depth), jnp.bfloat16),
            pltpu.VMEM((planes * depth, cells), jnp.bfloat16),
            pltpu.VMEM((groups * span, planes * depth), jnp.bfloat16),
            pltpu.VMEM((groups * span, cells // 2), jnp.float32),
            pltpu.VMEM((2, nz, groups, fac * NT_DEV, cells // 2), jnp.bfloat16),
            dma((nz,)),
            dma((nz,)),
            dma((nz,)),
            dma((nz,)),
            dma((nz,)),
            dma((nz,)),
            dma((nz,)),
            dma((nz,)),
            dma((pairs, nz)),
            dma((pairs, nz)),
            dma((pairs, nz)),
            dma((pairs, nz)),
            dma((pairs, nz)),
            dma((pairs, nz)),
            dma((nz, 2)),
            dma((nz, 2)),
            dma((nz + 2,)),
            dma,
        ],
        compiler_params=pltpu.CompilerParams(
            collective_id=0, has_side_effects=True, vmem_limit_bytes=60 * 1024 * 1024
        ),
    )(
        neighbours.T,
        counts,
        vis,
        delays.reshape(fac, pairs, 2, blk, lanes),
        tile_of,
        plane_of,
        kernels.reshape(planes * depth, cells),
    )
    spread = out.reshape(nz * groups, fac, NT_DEV, cells).astype(jnp.float32)
    return jnp.transpose(spread, (2, 1, 0, 3))


def solution(mesh):
    return jax.shard_map(
        local,
        mesh=mesh,
        in_specs=(
            P(None, None, None, ("facet", "chan"), None),
            P(),
            P("facet", None, None),
            P("facet", None),
            P("facet", None),
            P("facet"),
            P(),
        ),
        out_specs=P("chan", "facet", None, None),
        check_vma=False,
    )
```

```python
import functools
import math

import jax
import jax.numpy as jnp
from jax import lax
from jax.experimental import pallas as pl
from jax.experimental.pallas import tpu as pltpu
from jax.sharding import PartitionSpec as P

AVG = 8
TS = 16
NT_DEV = 16
EDGE = 4
LANES = 128
JOINED = 3
ORDER = (3, 0, 1, 2)
MESH = pl.DeviceIdType.MESH


def series(first, count, scale):
    return [
        (-1.0) ** i * scale ** (2 * i + first) / math.factorial(2 * i + first)
        for i in range(count)
    ]


SIN_HALF = series(1, 7, math.pi)
COS_HALF = series(0, 7, math.pi)


def turn_parts(turns):
    frac = turns - jnp.round(turns)
    square = frac * frac
    sine = jnp.full_like(frac, SIN_HALF[-1])
    cosine = jnp.full_like(frac, COS_HALF[-1])
    for a, b in zip(SIN_HALF[-2::-1], COS_HALF[-2::-1]):
        sine = sine * square + a
        cosine = cosine * square + b
    sine = sine * frac
    return 1.0 - 2.0 * sine * sine, 2.0 * sine * cosine


def flip(index, mask):
    bit = 1
    while bit <= mask:
        if mask & bit:
            index = index + bit - 2 * bit * lax.rem(index // bit, 2)
        bit *= 2
    return index


def kernel(
    cfg,
    neigh_ref,
    count_ref,
    vis_ref,
    delay_ref,
    tile_ref,
    plane_ref,
    kern_ref,
    out_ref,
    pair,
    part,
    got,
    raw,
    wide,
    rough,
    turns,
    codes,
    rows,
    kern,
    lhs,
    grid,
    final,
    mate_send,
    mate_recv,
    rough_send,
    rough_recv,
    turn_send,
    turn_recv,
    code_send,
    code_recv,
    part_send,
    part_recv,
    raw_send,
    raw_recv,
    row_send,
    row_recv,
    relay_send,
    relay_recv,
    fin_send,
    fin_recv,
    own_sem,
    kern_sem,
):
    n, nz, facets, fac, blk, groups, planes, tiles, joined, order = cfg
    me = lax.axis_index("chan")
    zme = lax.axis_index("facet")
    channels = groups * AVG * nz
    tile = kern_ref.shape[1] // 2
    edge = EDGE * TS
    pairs = n // 2
    parity = lax.rem(me, 2)
    mate = me + 1 - 2 * parity
    my_pair = me // 2
    half_avg = AVG // 2
    chunk_z = [flip(zme, c) for c in range(nz)]

    def group_of(c):
        return pl.ds(chunk_z[c] * fac, fac)

    load_kern = pltpu.make_async_copy(kern_ref, kern, kern_sem)
    own_wide = pltpu.make_async_copy(delay_ref.at[:, :, parity], wide, own_sem.at[nz])
    own_turns = pltpu.make_async_copy(
        delay_ref.at[:, my_pair, parity], turns.at[zme], own_sem.at[nz + 1]
    )

    def own_copy(c):
        if c >= joined:
            return pltpu.make_async_copy(
                vis_ref.at[:, group_of(c), my_pair, parity],
                raw.at[me, :, group_of(c)],
                own_sem.at[c],
            )
        return pltpu.make_async_copy(
            vis_ref.at[:, group_of(c), :, parity],
            pair.at[parity, :, group_of(c)],
            own_sem.at[c],
        )

    barrier = pltpu.get_barrier_semaphore()
    for d in range(1, n):
        pl.semaphore_signal(
            barrier, inc=1, device_id={"chan": lax.rem(me + d, n)}, device_id_type=MESH
        )
    for d in range(1, nz):
        pl.semaphore_signal(
            barrier, inc=1, device_id={"facet": chunk_z[d]}, device_id_type=MESH
        )
    own_wide.start()
    for c in range(nz):
        own_copy(c).start()
    own_turns.start()
    load_kern.start()

    blocks = blk * n
    block_id = lax.broadcasted_iota(jnp.int32, (1, blocks), 1)
    for i in range(fac):
        codes[zme, i : i + 1] = jnp.where(
            block_id < count_ref[i],
            plane_ref[i : i + 1] * tiles + tile_ref[i : i + 1],
            -1,
        )
    own_wide.wait()
    rough[zme] = wide[...].astype(jnp.bfloat16)
    pl.semaphore_wait(barrier, n + nz - 2)

    def mate_copy(c, slot):
        return pltpu.make_async_remote_copy(
            src_ref=vis_ref.at[:, group_of(c), :, 1 - parity],
            dst_ref=pair.at[slot, :, group_of(c)],
            send_sem=mate_send.at[c],
            recv_sem=mate_recv.at[c],
            device_id={"chan": mate},
            device_id_type=MESH,
        )

    def facet_copy(src, buffer, slot, d, send, recv):
        return pltpu.make_async_remote_copy(
            src_ref=src,
            dst_ref=buffer.at[slot],
            send_sem=send.at[d],
            recv_sem=recv.at[d],
            device_id={"facet": chunk_z[d]},
            device_id_type=MESH,
        )

    def rough_copy(d, slot):
        return facet_copy(rough.at[zme], rough, slot, d, rough_send, rough_recv)

    def turn_copy(d, slot):
        return facet_copy(
            delay_ref.at[:, my_pair, parity], turns, slot, d, turn_send, turn_recv
        )

    def code_copy(d, slot):
        return facet_copy(codes.at[zme], codes, slot, d, code_send, code_recv)

    def raw_copy(c, d, slot):
        peer = lax.rem(me + d, n)
        return pltpu.make_async_remote_copy(
            src_ref=vis_ref.at[:, group_of(c), peer // 2, lax.rem(peer, 2)],
            dst_ref=raw.at[slot, :, group_of(c)],
            send_sem=raw_send.at[d, c],
            recv_sem=raw_recv.at[d, c],
            device_id={"chan": peer},
            device_id_type=MESH,
        )

    for c in range(joined):
        mate_copy(c, parity).start()
    for c in order:
        if 0 < c < joined:
            rough_copy(c, zme).start()
        if c:
            turn_copy(c, zme).start()
        if c >= joined:
            for d in range(1, n):
                raw_copy(c, d, me).start()
    for d in range(1, nz):
        code_copy(d, zme).start()

    my_blocks = pl.ds(pl.multiple_of(me * blk, blk), blk)

    def part_copy(c, d, owner, slot):
        return pltpu.make_async_remote_copy(
            src_ref=part.at[owner, :, group_of(c)],
            dst_ref=got.at[slot, :, group_of(c)],
            send_sem=part_send.at[d, c],
            recv_sem=part_recv.at[d, c],
            device_id={"chan": 2 * owner + parity},
            device_id_type=MESH,
        )

    def row_copy(owner, peer, c, send, recv):
        piece = rows.at[group_of(c), pl.ds(pl.multiple_of(owner * blk, blk), blk)]
        return pltpu.make_async_remote_copy(
            src_ref=piece,
            dst_ref=piece,
            send_sem=send,
            recv_sem=recv,
            device_id={"chan": peer},
            device_id_type=MESH,
        )

    def after(d):
        return lax.rem(my_pair + d, pairs)

    def before(d):
        return lax.rem(my_pair + pairs - d, pairs)

    def join_pair(c):
        if c >= joined:
            return
        own_copy(c).wait()
        mate_copy(c, 1 - parity).wait_recv()
        if c:
            rough_copy(c, chunk_z[c]).wait_recv()

        def one(i, carry):
            slot = i // pairs
            q = lax.rem(i, pairs)
            f = chunk_z[c] * fac + slot
            delay = rough[chunk_z[c], slot, q].astype(jnp.float32) if c else wide[slot, q]
            cosine, sine = turn_parts(delay * (0.5 / channels))
            real = pair[1, 0, f, q].astype(jnp.float32)
            imag = pair[1, 1, f, q].astype(jnp.float32)
            part[q, 0, f] = (
                pair[0, 0, f, q].astype(jnp.float32) + (real * cosine - imag * sine)
            ).astype(jnp.bfloat16)
            part[q, 1, f] = (
                pair[0, 1, f, q].astype(jnp.float32) + (real * sine + imag * cosine)
            ).astype(jnp.bfloat16)
            return carry

        lax.fori_loop(0, fac * pairs, one, 0)
        for d in range(1, pairs):
            part_copy(c, d, after(d), my_pair).start()
        got[my_pair, :, group_of(c)] = part[my_pair, :, group_of(c)]

    def rotate(c):
        if c:
            turn_copy(c, chunk_z[c]).wait_recv()
        else:
            own_turns.wait()
        if c < joined:
            for d in range(1, pairs):
                part_copy(c, d, after(d), before(d)).wait_recv()
            source, terms = got, half_avg
        else:
            own_copy(c).wait()
            for d in range(1, n):
                raw_copy(c, d, lax.rem(me + n - d, n)).wait_recv()
            source, terms = raw, AVG
        step_turns = 0.5 * AVG / (terms * channels)

        def one(i, carry):
            f = chunk_z[c] * fac + i
            delay = turns[chunk_z[c], i]
            step_cos, step_sin = turn_parts(delay * step_turns)
            for g in range(groups):
                first = (zme * groups + g) * AVG
                start_cos, start_sin = turn_parts(
                    delay * (1.0 + (0.5 / channels) * first.astype(jnp.float32))
                )
                top = (g + 1) * terms - 1
                real = source[top, 0, f].astype(jnp.float32)
                imag = source[top, 1, f].astype(jnp.float32)
                for k in range(top - 1, g * terms - 1, -1):
                    next_real = source[k, 0, f].astype(jnp.float32) + (
                        real * step_cos - imag * step_sin
                    )
                    imag = source[k, 1, f].astype(jnp.float32) + (
                        real * step_sin + imag * step_cos
                    )
                    real = next_real
                rows[f, my_blocks, 2 * LANES * g : 2 * LANES * g + LANES] = (
                    (real * start_cos - imag * start_sin) * (1.0 / AVG)
                ).astype(jnp.bfloat16)
                rows[f, my_blocks, 2 * LANES * g + LANES : 2 * LANES * (g + 1)] = (
                    (real * start_sin + imag * start_cos) * (1.0 / AVG)
                ).astype(jnp.bfloat16)
            return carry

        lax.fori_loop(0, fac, one, 0)
        for q in range(1, pairs):
            row_copy(me, 2 * after(q) + parity, c, row_send.at[q, c], row_recv.at[q, c]).start()
        row_copy(me, mate, c, row_send.at[0, c], row_recv.at[0, c]).start()

    def relay(c):
        for q in range(1, pairs):
            owner = 2 * before(q) + parity
            row_copy(owner, mate, c, row_send.at[q, c], row_recv.at[q, c]).wait_recv()
            row_copy(owner, mate, c, relay_send.at[q, c], relay_recv.at[q, c]).start()

    entry = lax.broadcasted_iota(jnp.int32, (planes * NT_DEV, blocks), 0)
    wanted = (entry // NT_DEV) * tiles + me * NT_DEV + lax.rem(entry, NT_DEV)

    def gather_rows(c):
        if c:
            code_copy(c, chunk_z[c]).wait_recv()
        row_copy(mate, mate, c, row_send.at[0, c], row_recv.at[0, c]).wait_recv()
        for q in range(1, pairs):
            owner = 2 * before(q) + 1 - parity
            row_copy(owner, mate, c, relay_send.at[q, c], relay_recv.at[q, c]).wait_recv()
        for i in range(fac):
            f = chunk_z[c] * fac + i
            code = codes[chunk_z[c], i : i + 1]
            table = (code == wanted).astype(jnp.float32).astype(jnp.bfloat16)
            summed = jnp.dot(table, rows[f], preferred_element_type=jnp.float32).astype(
                jnp.bfloat16
            )
            for g in range(groups):
                at = pl.ds(pl.multiple_of((g * facets + f) * NT_DEV, NT_DEV), NT_DEV)
                for p in range(planes):
                    lhs[at, 2 * LANES * p : 2 * LANES * (p + 1)] = summed[
                        p * NT_DEV : (p + 1) * NT_DEV, 2 * LANES * g : 2 * LANES * (g + 1)
                    ]

    stages = (join_pair, rotate, relay, gather_rows)
    for step in range(nz + len(stages) - 1):
        for lag, stage in enumerate(stages):
            if 0 <= step - lag < nz:
                stage(order[step - lag])

    span = facets * NT_DEV
    row_id = lax.broadcasted_iota(jnp.int32, (NT_DEV, span), 0)
    col_id = lax.broadcasted_iota(jnp.int32, (NT_DEV, span), 1)
    same_tile = lax.rem(col_id, NT_DEV) == row_id
    col_facet = col_id // NT_DEV
    weights = []
    for f in range(facets):
        weight = jnp.zeros((NT_DEV, span), jnp.float32)
        for k in range(neigh_ref.shape[0]):
            weight += jnp.where(same_tile & (col_facet == neigh_ref[k, f]), 0.25, 0.0)
        weights.append(weight)
    mix = jnp.concatenate(weights, axis=0).astype(jnp.bfloat16)
    keep = lax.broadcasted_iota(jnp.int32, (span, LANES), 1) >= LANES - edge

    def fin_copy(half, d, slot):
        return pltpu.make_async_remote_copy(
            src_ref=final.at[half, chunk_z[d]],
            dst_ref=out_ref.at[slot, :, :, pl.ds(half * tile, tile)],
            send_sem=fin_send.at[d, half],
            recv_sem=fin_recv.at[d, half],
            device_id={"facet": chunk_z[d]},
            device_id_type=MESH,
        )

    load_kern.wait()
    for half in range(2):
        grid[...] = jnp.dot(
            lhs[...],
            kern[:, half * tile : (half + 1) * tile],
            preferred_element_type=jnp.float32,
        )
        for g in range(groups):
            here = slice(g * span, (g + 1) * span)
            blended = jnp.dot(
                mix, grid[here, :LANES].astype(jnp.bfloat16), preferred_element_type=jnp.float32
            )
            moved = pltpu.roll(blended, LANES - edge, 1)
            grid[here, tile - LANES :] += jnp.where(keep, moved, 0.0)
        for z in range(nz):
            for g in range(groups):
                at = (g * facets + z * fac) * NT_DEV
                final[half, z, g] = grid[at : at + fac * NT_DEV].astype(jnp.bfloat16)
        for d in range(1, nz):
            fin_copy(half, d, zme).start()
        out_ref[zme, :, :, half * tile : (half + 1) * tile] = final[half, zme]

    for c in range(nz):
        if c < joined:
            mate_copy(c, parity).wait_send()
            for d in range(1, pairs):
                part_copy(c, d, after(d), my_pair).wait_send()
        else:
            for d in range(1, n):
                raw_copy(c, d, me).wait_send()
        for q in range(pairs):
            row_copy(me, mate, c, row_send.at[q, c], row_recv.at[q, c]).wait_send()
        for q in range(1, pairs):
            row_copy(me, mate, c, relay_send.at[q, c], relay_recv.at[q, c]).wait_send()
    for d in range(1, nz):
        turn_copy(d, zme).wait_send()
        if d < joined:
            rough_copy(d, zme).wait_send()
        code_copy(d, zme).wait_send()
    for half in range(2):
        for d in range(1, nz):
            fin_copy(half, d, zme).wait_send()
            fin_copy(half, d, chunk_z[d]).wait_recv()


def local(visibilities, kernels, delays, tile_of, plane_of, counts, neighbours):
    n = lax.axis_size("chan")
    nz = lax.axis_size("facet")
    halves, facets, blocks, ch_dev, lanes = visibilities.shape
    planes, depth, cells = kernels.shape
    fac = facets // nz
    blk = blocks // n
    pairs = n // 2
    groups = n * ch_dev // AVG
    tiles = NT_DEV * n
    vis = visibilities.reshape(halves, facets, pairs, 2, blk, lanes)
    joined = min(JOINED, nz)
    order = ORDER if nz == len(ORDER) else tuple(range(nz))
    cfg = (n, nz, facets, fac, blk, groups, planes, tiles, joined, order)
    dma = pltpu.SemaphoreType.DMA
    span = facets * NT_DEV
    smem = pl.BlockSpec(memory_space=pltpu.SMEM)
    vmem = pl.BlockSpec(memory_space=pltpu.VMEM)
    anywhere = pl.BlockSpec(memory_space=pl.ANY)
    out = pl.pallas_call(
        functools.partial(kernel, cfg),
        out_shape=jax.ShapeDtypeStruct((nz, groups, fac * NT_DEV, cells), jnp.bfloat16),
        in_specs=[smem, smem, anywhere, anywhere, vmem, vmem, anywhere],
        out_specs=vmem,
        scratch_shapes=[
            pltpu.VMEM((2, halves, facets, pairs, blk, lanes), jnp.bfloat16),
            pltpu.VMEM((pairs, halves, facets, blk, lanes), jnp.bfloat16),
            pltpu.VMEM((pairs, halves, facets, blk, lanes), jnp.bfloat16),
            pltpu.VMEM((n, halves, facets, blk, lanes), jnp.bfloat16),
            pltpu.VMEM((fac, pairs, blk, lanes), jnp.float32),
            pltpu.VMEM((nz, fac, pairs, blk, lanes), jnp.bfloat16),
            pltpu.VMEM((nz, fac, blk, lanes), jnp.float32),
            pltpu.VMEM((nz, fac, blocks), jnp.int32),
            pltpu.VMEM((facets, blocks, groups * depth), jnp.bfloat16),
            pltpu.VMEM((planes * depth, cells), jnp.bfloat16),
            pltpu.VMEM((groups * span, planes * depth), jnp.bfloat16),
            pltpu.VMEM((groups * span, cells // 2), jnp.float32),
            pltpu.VMEM((2, nz, groups, fac * NT_DEV, cells // 2), jnp.bfloat16),
            dma((nz,)),
            dma((nz,)),
            dma((nz,)),
            dma((nz,)),
            dma((nz,)),
            dma((nz,)),
            dma((nz,)),
            dma((nz,)),
            dma((pairs, nz)),
            dma((pairs, nz)),
            dma((n, nz)),
            dma((n, nz)),
            dma((pairs, nz)),
            dma((pairs, nz)),
            dma((pairs, nz)),
            dma((pairs, nz)),
            dma((nz, 2)),
            dma((nz, 2)),
            dma((nz + 2,)),
            dma,
        ],
        compiler_params=pltpu.CompilerParams(
            collective_id=0, has_side_effects=True, vmem_limit_bytes=60 * 1024 * 1024
        ),
    )(
        neighbours.T,
        counts,
        vis,
        delays.reshape(fac, pairs, 2, blk, lanes),
        tile_of,
        plane_of,
        kernels.reshape(planes * depth, cells),
    )
    spread = out.reshape(nz * groups, fac, NT_DEV, cells).astype(jnp.float32)
    return jnp.transpose(spread, (2, 1, 0, 3))


def solution(mesh):
    return jax.shard_map(
        local,
        mesh=mesh,
        in_specs=(
            P(None, None, None, ("facet", "chan"), None),
            P(),
            P("facet", None, None),
            P("facet", None),
            P("facet", None),
            P("facet"),
            P(),
        ),
        out_specs=P("chan", "facet", None, None),
        check_vma=False,
    )
```

```python
import functools
import math

import jax
import jax.numpy as jnp
from jax import lax
from jax.experimental import pallas as pl
from jax.experimental.pallas import tpu as pltpu
from jax.sharding import PartitionSpec as P

AVG = 8
TS = 16
NT_DEV = 16
EDGE = 4
LANES = 128
JOINED = 3
ORDER = (3, 0, 1, 2)
MESH = pl.DeviceIdType.MESH


def series(first, count, scale):
    return [
        (-1.0) ** i * scale ** (2 * i + first) / math.factorial(2 * i + first)
        for i in range(count)
    ]


SIN_HALF = series(1, 7, math.pi)
COS_HALF = series(0, 7, math.pi)


def turn_parts(turns):
    frac = turns - jnp.round(turns)
    square = frac * frac
    sine = jnp.full_like(frac, SIN_HALF[-1])
    cosine = jnp.full_like(frac, COS_HALF[-1])
    for a, b in zip(SIN_HALF[-2::-1], COS_HALF[-2::-1]):
        sine = sine * square + a
        cosine = cosine * square + b
    sine = sine * frac
    return 1.0 - 2.0 * sine * sine, 2.0 * sine * cosine


def flip(index, mask):
    bit = 1
    while bit <= mask:
        if mask & bit:
            index = index + bit - 2 * bit * lax.rem(index // bit, 2)
        bit *= 2
    return index


def kernel(
    cfg,
    neigh_ref,
    count_ref,
    vis_ref,
    delay_ref,
    tile_ref,
    plane_ref,
    kern_ref,
    out_ref,
    pair,
    part,
    got,
    raw,
    wide,
    rough,
    turns,
    codes,
    rows,
    kern,
    lhs,
    grid,
    final,
    mate_send,
    mate_recv,
    rough_send,
    rough_recv,
    turn_send,
    turn_recv,
    code_send,
    code_recv,
    part_send,
    part_recv,
    raw_send,
    raw_recv,
    row_send,
    row_recv,
    relay_send,
    relay_recv,
    fin_send,
    fin_recv,
    own_sem,
    kern_sem,
):
    n, nz, facets, fac, blk, groups, planes, tiles, joined, order = cfg
    me = lax.axis_index("chan")
    zme = lax.axis_index("facet")
    channels = groups * AVG * nz
    tile = kern_ref.shape[1] // 2
    edge = EDGE * TS
    pairs = n // 2
    parity = lax.rem(me, 2)
    mate = me + 1 - 2 * parity
    my_pair = me // 2
    half_avg = AVG // 2
    chunk_z = [flip(zme, c) for c in range(nz)]

    def group_of(c):
        return pl.ds(chunk_z[c] * fac, fac)

    load_kern = pltpu.make_async_copy(kern_ref, kern, kern_sem)
    own_wide = pltpu.make_async_copy(delay_ref.at[:, :, parity], wide, own_sem.at[nz])
    own_turns = pltpu.make_async_copy(
        delay_ref.at[:, my_pair, parity], turns.at[zme], own_sem.at[nz + 1]
    )

    def own_copy(c):
        if c >= joined:
            return pltpu.make_async_copy(
                vis_ref.at[:, group_of(c), my_pair, parity],
                raw.at[me, :, group_of(c)],
                own_sem.at[c],
            )
        return pltpu.make_async_copy(
            vis_ref.at[:, group_of(c), :, parity],
            pair.at[parity, :, group_of(c)],
            own_sem.at[c],
        )

    barrier = pltpu.get_barrier_semaphore()
    for d in range(1, n):
        pl.semaphore_signal(
            barrier, inc=1, device_id={"chan": lax.rem(me + d, n)}, device_id_type=MESH
        )
    for d in range(1, nz):
        pl.semaphore_signal(
            barrier, inc=1, device_id={"facet": chunk_z[d]}, device_id_type=MESH
        )
    own_wide.start()
    for c in range(nz):
        own_copy(c).start()
    own_turns.start()
    load_kern.start()

    blocks = blk * n
    block_id = lax.broadcasted_iota(jnp.int32, (1, blocks), 1)
    for i in range(fac):
        codes[zme, i : i + 1] = jnp.where(
            block_id < count_ref[i],
            plane_ref[i : i + 1] * tiles + tile_ref[i : i + 1],
            -1,
        )
    own_wide.wait()
    rough[zme] = wide[...].astype(jnp.bfloat16)
    pl.semaphore_wait(barrier, n + nz - 2)

    def mate_copy(c, slot):
        return pltpu.make_async_remote_copy(
            src_ref=vis_ref.at[:, group_of(c), :, 1 - parity],
            dst_ref=pair.at[slot, :, group_of(c)],
            send_sem=mate_send.at[c],
            recv_sem=mate_recv.at[c],
            device_id={"chan": mate},
            device_id_type=MESH,
        )

    def facet_copy(src, buffer, slot, d, send, recv):
        return pltpu.make_async_remote_copy(
            src_ref=src,
            dst_ref=buffer.at[slot],
            send_sem=send.at[d],
            recv_sem=recv.at[d],
            device_id={"facet": chunk_z[d]},
            device_id_type=MESH,
        )

    def rough_copy(d, slot):
        return facet_copy(rough.at[zme], rough, slot, d, rough_send, rough_recv)

    def turn_copy(d, slot):
        return facet_copy(
            delay_ref.at[:, my_pair, parity], turns, slot, d, turn_send, turn_recv
        )

    def code_copy(d, slot):
        return facet_copy(codes.at[zme], codes, slot, d, code_send, code_recv)

    def raw_copy(c, d, slot):
        peer = lax.rem(me + d, n)
        return pltpu.make_async_remote_copy(
            src_ref=vis_ref.at[:, group_of(c), peer // 2, lax.rem(peer, 2)],
            dst_ref=raw.at[slot, :, group_of(c)],
            send_sem=raw_send.at[d, c],
            recv_sem=raw_recv.at[d, c],
            device_id={"chan": peer},
            device_id_type=MESH,
        )

    for c in range(joined):
        mate_copy(c, parity).start()
    for c in order:
        if 0 < c < joined:
            rough_copy(c, zme).start()
        if c:
            turn_copy(c, zme).start()
        if c >= joined:
            for d in range(1, n):
                raw_copy(c, d, me).start()
    for d in range(1, nz):
        code_copy(d, zme).start()

    my_blocks = pl.ds(pl.multiple_of(me * blk, blk), blk)

    def part_copy(c, d, owner, slot):
        return pltpu.make_async_remote_copy(
            src_ref=part.at[owner, :, group_of(c)],
            dst_ref=got.at[slot, :, group_of(c)],
            send_sem=part_send.at[d, c],
            recv_sem=part_recv.at[d, c],
            device_id={"chan": 2 * owner + parity},
            device_id_type=MESH,
        )

    def row_copy(owner, peer, c, send, recv):
        piece = rows.at[group_of(c), pl.ds(pl.multiple_of(owner * blk, blk), blk)]
        return pltpu.make_async_remote_copy(
            src_ref=piece,
            dst_ref=piece,
            send_sem=send,
            recv_sem=recv,
            device_id={"chan": peer},
            device_id_type=MESH,
        )

    def after(d):
        return lax.rem(my_pair + d, pairs)

    def before(d):
        return lax.rem(my_pair + pairs - d, pairs)

    def join_pair(c):
        if c >= joined:
            return
        own_copy(c).wait()
        mate_copy(c, 1 - parity).wait_recv()
        if c:
            rough_copy(c, chunk_z[c]).wait_recv()

        def one(i, carry):
            slot = i // pairs
            q = lax.rem(i, pairs)
            f = chunk_z[c] * fac + slot
            delay = rough[chunk_z[c], slot, q].astype(jnp.float32) if c else wide[slot, q]
            cosine, sine = turn_parts(delay * (0.5 / channels))
            real = pair[1, 0, f, q].astype(jnp.float32)
            imag = pair[1, 1, f, q].astype(jnp.float32)
            part[q, 0, f] = (
                pair[0, 0, f, q].astype(jnp.float32) + (real * cosine - imag * sine)
            ).astype(jnp.bfloat16)
            part[q, 1, f] = (
                pair[0, 1, f, q].astype(jnp.float32) + (real * sine + imag * cosine)
            ).astype(jnp.bfloat16)
            return carry

        lax.fori_loop(0, fac * pairs, one, 0)
        for d in range(1, pairs):
            part_copy(c, d, after(d), my_pair).start()
        got[my_pair, :, group_of(c)] = part[my_pair, :, group_of(c)]

    def rotate(c):
        if c:
            turn_copy(c, chunk_z[c]).wait_recv()
        else:
            own_turns.wait()
        if c < joined:
            for d in range(1, pairs):
                part_copy(c, d, after(d), before(d)).wait_recv()
            source, terms = got, half_avg
        else:
            own_copy(c).wait()
            for d in range(1, n):
                raw_copy(c, d, lax.rem(me + n - d, n)).wait_recv()
            source, terms = raw, AVG
        step_turns = 0.5 * AVG / (terms * channels)

        def one(i, carry):
            f = chunk_z[c] * fac + i
            delay = turns[chunk_z[c], i]
            step_cos, step_sin = turn_parts(delay * step_turns)
            for g in range(groups):
                first = (zme * groups + g) * AVG
                start_cos, start_sin = turn_parts(
                    delay * (1.0 + (0.5 / channels) * first.astype(jnp.float32))
                )
                top = (g + 1) * terms - 1
                real = source[top, 0, f].astype(jnp.float32)
                imag = source[top, 1, f].astype(jnp.float32)
                for k in range(top - 1, g * terms - 1, -1):
                    next_real = source[k, 0, f].astype(jnp.float32) + (
                        real * step_cos - imag * step_sin
                    )
                    imag = source[k, 1, f].astype(jnp.float32) + (
                        real * step_sin + imag * step_cos
                    )
                    real = next_real
                rows[f, my_blocks, 2 * LANES * g : 2 * LANES * g + LANES] = (
                    (real * start_cos - imag * start_sin) * (1.0 / AVG)
                ).astype(jnp.bfloat16)
                rows[f, my_blocks, 2 * LANES * g + LANES : 2 * LANES * (g + 1)] = (
                    (real * start_sin + imag * start_cos) * (1.0 / AVG)
                ).astype(jnp.bfloat16)
            return carry

        lax.fori_loop(0, fac, one, 0)
        for q in range(1, pairs):
            row_copy(me, 2 * after(q) + parity, c, row_send.at[q, c], row_recv.at[q, c]).start()
        row_copy(me, mate, c, row_send.at[0, c], row_recv.at[0, c]).start()

    def relay(c):
        for q in range(1, pairs):
            owner = 2 * before(q) + parity
            row_copy(owner, mate, c, row_send.at[q, c], row_recv.at[q, c]).wait_recv()
            row_copy(owner, mate, c, relay_send.at[q, c], relay_recv.at[q, c]).start()

    entry = lax.broadcasted_iota(jnp.int32, (planes * NT_DEV, blocks), 0)
    wanted = (entry // NT_DEV) * tiles + me * NT_DEV + lax.rem(entry, NT_DEV)

    def gather_rows(c):
        if c:
            code_copy(c, chunk_z[c]).wait_recv()
        tables = [
            (codes[chunk_z[c], i : i + 1] == wanted).astype(jnp.float32).astype(jnp.bfloat16)
            for i in range(fac)
        ]
        row_copy(mate, mate, c, row_send.at[0, c], row_recv.at[0, c]).wait_recv()
        for q in range(1, pairs):
            owner = 2 * before(q) + 1 - parity
            row_copy(owner, mate, c, relay_send.at[q, c], relay_recv.at[q, c]).wait_recv()
        for i in range(fac):
            f = chunk_z[c] * fac + i
            summed = jnp.dot(tables[i], rows[f], preferred_element_type=jnp.float32).astype(
                jnp.bfloat16
            )
            for g in range(groups):
                at = pl.ds(pl.multiple_of((g * facets + f) * NT_DEV, NT_DEV), NT_DEV)
                for p in range(planes):
                    lhs[at, 2 * LANES * p : 2 * LANES * (p + 1)] = summed[
                        p * NT_DEV : (p + 1) * NT_DEV, 2 * LANES * g : 2 * LANES * (g + 1)
                    ]

    span = facets * NT_DEV
    row_id = lax.broadcasted_iota(jnp.int32, (NT_DEV, span), 0)
    col_id = lax.broadcasted_iota(jnp.int32, (NT_DEV, span), 1)
    same_tile = lax.rem(col_id, NT_DEV) == row_id
    col_facet = col_id // NT_DEV
    weights = []
    for f in range(facets):
        weight = jnp.zeros((NT_DEV, span), jnp.float32)
        for k in range(neigh_ref.shape[0]):
            weight += jnp.where(same_tile & (col_facet == neigh_ref[k, f]), 0.25, 0.0)
        weights.append(weight)
    mix = jnp.concatenate(weights, axis=0).astype(jnp.bfloat16)
    keep = lax.broadcasted_iota(jnp.int32, (span, LANES), 1) >= LANES - edge

    stages = (join_pair, rotate, relay, gather_rows)
    for step in range(nz + len(stages) - 1):
        for lag, stage in enumerate(stages):
            if 0 <= step - lag < nz:
                stage(order[step - lag])

    def fin_copy(half, d, slot):
        return pltpu.make_async_remote_copy(
            src_ref=final.at[half, chunk_z[d]],
            dst_ref=out_ref.at[slot, :, :, pl.ds(half * tile, tile)],
            send_sem=fin_send.at[d, half],
            recv_sem=fin_recv.at[d, half],
            device_id={"facet": chunk_z[d]},
            device_id_type=MESH,
        )

    load_kern.wait()
    for half in range(2):
        grid[...] = jnp.dot(
            lhs[...],
            kern[:, half * tile : (half + 1) * tile],
            preferred_element_type=jnp.float32,
        )
        for g in range(groups):
            here = slice(g * span, (g + 1) * span)
            blended = jnp.dot(
                mix, grid[here, :LANES].astype(jnp.bfloat16), preferred_element_type=jnp.float32
            )
            moved = pltpu.roll(blended, LANES - edge, 1)
            grid[here, tile - LANES :] += jnp.where(keep, moved, 0.0)
        for z in range(nz):
            for g in range(groups):
                at = (g * facets + z * fac) * NT_DEV
                final[half, z, g] = grid[at : at + fac * NT_DEV].astype(jnp.bfloat16)
        for d in range(1, nz):
            fin_copy(half, d, zme).start()
        out_ref[zme, :, :, half * tile : (half + 1) * tile] = final[half, zme]

    for c in range(nz):
        if c < joined:
            mate_copy(c, parity).wait_send()
            for d in range(1, pairs):
                part_copy(c, d, after(d), my_pair).wait_send()
        else:
            for d in range(1, n):
                raw_copy(c, d, me).wait_send()
        for q in range(pairs):
            row_copy(me, mate, c, row_send.at[q, c], row_recv.at[q, c]).wait_send()
        for q in range(1, pairs):
            row_copy(me, mate, c, relay_send.at[q, c], relay_recv.at[q, c]).wait_send()
    for d in range(1, nz):
        turn_copy(d, zme).wait_send()
        if d < joined:
            rough_copy(d, zme).wait_send()
        code_copy(d, zme).wait_send()
    for half in range(2):
        for d in range(1, nz):
            fin_copy(half, d, zme).wait_send()
            fin_copy(half, d, chunk_z[d]).wait_recv()


def local(visibilities, kernels, delays, tile_of, plane_of, counts, neighbours):
    n = lax.axis_size("chan")
    nz = lax.axis_size("facet")
    halves, facets, blocks, ch_dev, lanes = visibilities.shape
    planes, depth, cells = kernels.shape
    fac = facets // nz
    blk = blocks // n
    pairs = n // 2
    groups = n * ch_dev // AVG
    tiles = NT_DEV * n
    vis = visibilities.reshape(halves, facets, pairs, 2, blk, lanes)
    joined = min(JOINED, nz)
    order = ORDER if nz == len(ORDER) else tuple(range(nz))
    cfg = (n, nz, facets, fac, blk, groups, planes, tiles, joined, order)
    dma = pltpu.SemaphoreType.DMA
    span = facets * NT_DEV
    smem = pl.BlockSpec(memory_space=pltpu.SMEM)
    vmem = pl.BlockSpec(memory_space=pltpu.VMEM)
    anywhere = pl.BlockSpec(memory_space=pl.ANY)
    out = pl.pallas_call(
        functools.partial(kernel, cfg),
        out_shape=jax.ShapeDtypeStruct((nz, groups, fac * NT_DEV, cells), jnp.bfloat16),
        in_specs=[smem, smem, anywhere, anywhere, vmem, vmem, anywhere],
        out_specs=vmem,
        scratch_shapes=[
            pltpu.VMEM((2, halves, facets, pairs, blk, lanes), jnp.bfloat16),
            pltpu.VMEM((pairs, halves, facets, blk, lanes), jnp.bfloat16),
            pltpu.VMEM((pairs, halves, facets, blk, lanes), jnp.bfloat16),
            pltpu.VMEM((n, halves, facets, blk, lanes), jnp.bfloat16),
            pltpu.VMEM((fac, pairs, blk, lanes), jnp.float32),
            pltpu.VMEM((nz, fac, pairs, blk, lanes), jnp.bfloat16),
            pltpu.VMEM((nz, fac, blk, lanes), jnp.float32),
            pltpu.VMEM((nz, fac, blocks), jnp.int32),
            pltpu.VMEM((facets, blocks, groups * depth), jnp.bfloat16),
            pltpu.VMEM((planes * depth, cells), jnp.bfloat16),
            pltpu.VMEM((groups * span, planes * depth), jnp.bfloat16),
            pltpu.VMEM((groups * span, cells // 2), jnp.float32),
            pltpu.VMEM((2, nz, groups, fac * NT_DEV, cells // 2), jnp.bfloat16),
            dma((nz,)),
            dma((nz,)),
            dma((nz,)),
            dma((nz,)),
            dma((nz,)),
            dma((nz,)),
            dma((nz,)),
            dma((nz,)),
            dma((pairs, nz)),
            dma((pairs, nz)),
            dma((n, nz)),
            dma((n, nz)),
            dma((pairs, nz)),
            dma((pairs, nz)),
            dma((pairs, nz)),
            dma((pairs, nz)),
            dma((nz, 2)),
            dma((nz, 2)),
            dma((nz + 2,)),
            dma,
        ],
        compiler_params=pltpu.CompilerParams(
            collective_id=0, has_side_effects=True, vmem_limit_bytes=60 * 1024 * 1024
        ),
    )(
        neighbours.T,
        counts,
        vis,
        delays.reshape(fac, pairs, 2, blk, lanes),
        tile_of,
        plane_of,
        kernels.reshape(planes * depth, cells),
    )
    spread = out.reshape(nz * groups, fac, NT_DEV, cells).astype(jnp.float32)
    return jnp.transpose(spread, (2, 1, 0, 3))


def solution(mesh):
    return jax.shard_map(
        local,
        mesh=mesh,
        in_specs=(
            P(None, None, None, ("facet", "chan"), None),
            P(),
            P("facet", None, None),
            P("facet", None),
            P("facet", None),
            P("facet"),
            P(),
        ),
        out_specs=P("chan", "facet", None, None),
        check_vma=False,
    )
```
